32 devices in a mesh: par: 4 (over x, core), freq: 8 (over z, y).
Axes of the slice: x: 2, y: 2, z: 4, core: 2. Of those that a mesh axis runs over, the one named last changes fastest.
Arguments:
- probes: bfloat16 [64, 600, 420], P('freq'), may hold values from -6 to 6
- map_real: bfloat16 [112, 600, 1024], P('freq', None, 'par'), may hold values from -0.1875 to 0.1875
- map_imag: bfloat16 [112, 600, 1024], P('freq', None, 'par'), may hold values from -0.1875 to 0.1875
- prior_var: float32 [1024], P('par'), may hold values from 0.05 to 13, as said below
Outputs:
- applied: bfloat16 [64, 600, 420], P('freq')
The draws below stay inside these ranges and needn't reach their ends.
Inputs may be any that keep to these rules, and one draw needn't show every extreme that they name: `prior_var`: prior variances are positive.
All inputs are finite; a program needn't handle non-finite values.
Results may differ from the reference program's by a relative error of at most 0.014.
Values may be sent and summed in bfloat16 or wider, within the bound.
A program may use at most 64 MiB of HBM per device.

```python
import jax
import jax.numpy as jnp
from jax import lax

SENSORS = 600
STEPS = 420
PERIOD = 840
PARAMS = 1024
BINS = 112
PROBES = 64


def draw_prior_var(key, part):
    position = jnp.arange(PARAMS, dtype=jnp.float32) / PARAMS
    ramp = jnp.exp(jnp.log(8.0) * position) / 3.0
    rough = jnp.exp(jax.random.uniform(key, (PARAMS,), jnp.float32, jnp.log(0.5), jnp.log(2.0)))
    return (ramp * rough).astype(jnp.float32)


def block_scale(stream_key, extent, split, low, top_value):
    loudness, own = 1.0, jax.random.fold_in(stream_key, 6)
    for axis_at, blocks in split:
        draws = jnp.exp(jax.random.uniform(jax.random.fold_in(own, axis_at), (blocks,), jnp.float32, low / len(split), top_value / len(split)))
        loudness = loudness * jnp.repeat(draws, extent[axis_at] // blocks).reshape([-1 if axis == axis_at else 1 for axis in range(len(extent))])
    return loudness


def bell_draw(key, dims, width, reach, pieces=(), kind=jnp.bfloat16):
    gain = block_scale(key, dims, pieces, -0.22, 0.18) if pieces else 1.0
    values = jax.random.normal(key, dims, jnp.float32) * width * gain
    return jnp.minimum(jnp.maximum(values, -reach), reach).astype(kind)


def setup_inputs(seed: int = 0) -> dict:
    key_list = jax.random.split(jax.random.key(seed), 5)
    probes = bell_draw(key_list[0], (PROBES, SENSORS, STEPS), 1.0, 6.0, ((0, 8),))
    map_real = bell_draw(key_list[1], (BINS, SENSORS, PARAMS), PARAMS ** -0.5, 0.1875, ((0, 8), (2, 4)))
    map_imag = bell_draw(key_list[2], (BINS, SENSORS, PARAMS), PARAMS ** -0.5, 0.1875, ((0, 8), (2, 4)))
    prior_var = draw_prior_var(jax.random.fold_in(key_list[4], 71), 0)
    return dict(probes=probes, map_real=map_real, map_imag=map_imag, prior_var=prior_var)


noise_ratio = 0.5

def reference(probes, map_real, map_imag, prior_var):
    time_steps = jnp.arange(STEPS, dtype=jnp.int32)
    bin_index = jnp.arange(BINS, dtype=jnp.int32)
    product_index = time_steps[:, None] * bin_index[None, :] % PERIOD
    angles = product_index.astype(jnp.float32) * (2.0 * jnp.pi / PERIOD)
    norm_scale = 1.0 / jnp.sqrt(jnp.float32(PERIOD))
    cosines = jnp.cos(angles) * norm_scale
    sines = jnp.sin(angles) * norm_scale
    bin_weight = jnp.where(bin_index == 0, 1.0, 2.0).astype(jnp.float32)
    flattened = probes.astype(jnp.float32).reshape(PROBES * SENSORS, STEPS)
    spec_real = jnp.dot(flattened, cosines, precision=lax.Precision.HIGHEST)
    spec_imag = -jnp.dot(flattened, sines, precision=lax.Precision.HIGHEST)
    spec_real = spec_real.astype(jnp.bfloat16).reshape(PROBES, SENSORS, BINS).transpose(2, 1, 0)
    spec_imag = spec_imag.astype(jnp.bfloat16).reshape(PROBES, SENSORS, BINS).transpose(2, 1, 0)
    spectra = jnp.concatenate([spec_real, spec_imag], axis=-1)

    def per_bin(items):
        real_block, imag_block, spec_block, weight_one = items
        left_real = jnp.dot(real_block.T, spec_block, preferred_element_type=jnp.float32)
        left_imag = jnp.dot(imag_block.T, spec_block, preferred_element_type=jnp.float32)
        u_real = left_real[:, :PROBES] + left_imag[:, PROBES:]
        u_imag = left_real[:, PROBES:] - left_imag[:, :PROBES]
        quadratic = weight_one * jnp.sum(prior_var[:, None] * (u_real * u_real + u_imag * u_imag))
        scaled = (jnp.concatenate([u_real, u_imag], axis=-1) * prior_var[:, None]).astype(jnp.bfloat16)
        right_real = jnp.dot(real_block, scaled, preferred_element_type=jnp.float32)
        right_imag = jnp.dot(imag_block, scaled, preferred_element_type=jnp.float32)
        w_real = right_real[:, :PROBES] - right_imag[:, PROBES:]
        w_imag = right_real[:, PROBES:] + right_imag[:, :PROBES]
        return (jnp.concatenate([w_real, w_imag], axis=-1).astype(jnp.bfloat16), quadratic)
    responses, quadratics = lax.map(per_bin, (map_real, map_imag, spectra, bin_weight))
    trace_est = jnp.sum(quadratics) / (PROBES * SENSORS * STEPS)
    responses = responses.astype(jnp.float32)
    w_real = responses[:, :, :PROBES].transpose(2, 1, 0).reshape(PROBES * SENSORS, BINS)
    w_imag = responses[:, :, PROBES:].transpose(2, 1, 0).reshape(PROBES * SENSORS, BINS)
    cos_weighted = (cosines * bin_weight[None, :]).T
    sin_weighted = (sines * bin_weight[None, :]).T
    response = jnp.dot(w_real, cos_weighted, precision=lax.Precision.HIGHEST) - jnp.dot(w_imag, sin_weighted, precision=lax.Precision.HIGHEST)
    response = response.reshape(PROBES, SENSORS, STEPS)
    return (response + noise_ratio * trace_est * probes.astype(jnp.float32)).astype(jnp.bfloat16)
```

```python
import functools

import jax
import jax.numpy as jnp
import numpy as np
from jax import lax
from jax.experimental import pallas as pl
from jax.experimental.pallas import tpu as pltpu
from jax.sharding import PartitionSpec as P

SENSORS = 600
STEPS = 420
PERIOD = 840
PROBES = 64


noise_ratio = 0.5


def split_product(left, table):
    upper = table.astype(jnp.bfloat16)
    lower = (table - upper.astype(jnp.float32)).astype(jnp.bfloat16)
    return jnp.dot(left, upper, preferred_element_type=jnp.float32) + jnp.dot(
        left, lower, preferred_element_type=jnp.float32
    )


def plain_shards(probes, map_real, map_imag, prior_var):
    freq_count = lax.axis_size("freq")
    bins_dev = map_real.shape[0]
    probe_block = probes.shape[0]
    total_bins = bins_dev * freq_count
    time_steps = jnp.arange(STEPS, dtype=jnp.int32)
    bin_index = jnp.arange(total_bins, dtype=jnp.int32)
    product_index = time_steps[:, None] * bin_index[None, :] % PERIOD
    angles = product_index.astype(jnp.float32) * (2.0 * jnp.pi / PERIOD)
    norm_scale = 1.0 / jnp.sqrt(jnp.float32(PERIOD))
    cosines = jnp.cos(angles) * norm_scale
    sines = jnp.sin(angles) * norm_scale
    forward = jnp.stack([cosines, -sines], axis=2).reshape(STEPS, 2 * total_bins)
    all_weight = jnp.where(bin_index == 0, 1.0, 2.0).astype(jnp.float32)
    inverse = jnp.stack([cosines * all_weight[None, :], -sines * all_weight[None, :]], axis=2)
    inverse = inverse.reshape(STEPS, 2 * total_bins).T
    flattened = probes.reshape(probe_block * SENSORS, STEPS)
    spectrum = split_product(flattened, forward).astype(jnp.bfloat16)
    spectrum = spectrum.reshape(probe_block, SENSORS, 2 * total_bins)
    exchanged = lax.all_to_all(spectrum, "freq", split_axis=2, concat_axis=0, tiled=True)
    all_probes = exchanged.shape[0]
    operand = exchanged.reshape(all_probes, SENSORS, bins_dev, 2).transpose(2, 1, 3, 0)
    operand = operand.reshape(bins_dev, SENSORS, 2 * all_probes)
    left_real = jnp.einsum("ksp,ksc->kpc", map_real, operand, preferred_element_type=jnp.float32)
    left_imag = jnp.einsum("ksp,ksc->kpc", map_imag, operand, preferred_element_type=jnp.float32)
    u_real = left_real[..., :all_probes] + left_imag[..., all_probes:]
    u_imag = left_real[..., all_probes:] - left_imag[..., :all_probes]
    global_bin = lax.axis_index("freq") * bins_dev + jnp.arange(bins_dev, dtype=jnp.int32)
    bin_weight = jnp.where(global_bin == 0, 1.0, 2.0).astype(jnp.float32)
    quadratic = jnp.sum(
        bin_weight[:, None, None] * prior_var[None, :, None] * (u_real * u_real + u_imag * u_imag)
    )
    trace_est = lax.psum(quadratic, ("par", "freq")) / (PROBES * SENSORS * STEPS)
    scaled = (jnp.concatenate([u_real, u_imag], axis=-1) * prior_var[None, :, None]).astype(
        jnp.bfloat16
    )
    right_real = jnp.einsum("ksp,kpc->ksc", map_real, scaled, preferred_element_type=jnp.float32)
    right_imag = jnp.einsum("ksp,kpc->ksc", map_imag, scaled, preferred_element_type=jnp.float32)
    w_partial = jnp.concatenate(
        [
            right_real[..., :all_probes] - right_imag[..., all_probes:],
            right_real[..., all_probes:] + right_imag[..., :all_probes],
        ],
        axis=-1,
    )
    summed = lax.psum(w_partial.astype(jnp.bfloat16), "par")
    outgoing = summed.reshape(bins_dev, SENSORS, 2, all_probes).transpose(3, 1, 0, 2)
    outgoing = outgoing.reshape(all_probes, SENSORS, 2 * bins_dev)
    by_probe = lax.all_to_all(outgoing, "freq", split_axis=0, concat_axis=2, tiled=True)
    by_rows = by_probe.reshape(probe_block * SENSORS, 2 * total_bins)
    response = split_product(by_rows, inverse).reshape(probe_block, SENSORS, STEPS)
    return (response + noise_ratio * trace_est * probes.astype(jnp.float32)).astype(jnp.bfloat16)


MESH = pl.DeviceIdType.MESH
ROWS = 16
STAGES = 4
F32, BF16 = jnp.float32, jnp.bfloat16


def tables(steps, bins_dev, freq_count, par_count):
    padded = STAGES * par_count
    local = np.arange(padded)
    bins = np.arange(freq_count)[:, None] * bins_dev + local[None, :]
    angle = 2.0 * np.pi * ((bins[:, :, None] * np.arange(steps)) % PERIOD) / PERIOD
    scale = (local < bins_dev)[None, :, None] / np.sqrt(PERIOD)
    both = np.stack([np.cos(angle) * scale, -np.sin(angle) * scale], axis=2)
    weight = np.where(bins == 0, 1.0, 2.0)[:, :, None, None]
    forward = both.reshape(freq_count, par_count, STAGES, 2, steps).transpose(1, 2, 0, 3, 4)
    forward = forward.reshape(par_count, STAGES * freq_count * 2, steps)
    inverse = (both * weight).reshape(freq_count * padded * 2, steps)
    return forward.astype(np.float32), inverse.astype(np.float32)


def swap_matrix(outer, inner):
    out = np.arange(outer * inner)
    matrix = np.zeros((out.size, out.size), np.float32)
    matrix[out, (out % outer) * inner + out // outer] = 1.0
    return matrix


def exchange_kernel(
    freq_count, table_ref, swap_ref, prior_ref, probes_hbm, real_hbm, imag_hbm, y_hbm, trace_ref,
    probes_v, real_v, imag_v, o_buf, s_buf, v_buf, w_buf, a_buf, h_buf, b_buf, q_buf, y_buf,
    t_own, t_freq, t_mid, t_core, t_half, t_x,
    load_sem, map_sem, out_sem, f_send, f_recv, g_send, g_recv, h_send, h_recv,
    r_send, r_recv, rx_send, rx_recv, bf_send, bf_recv, bg_send, bg_recv, bh_send, bh_recv,
    t_send, t_recv, tp_send, tp_recv,
):
    par, freq = lax.axis_index("par"), lax.axis_index("freq")
    core, side = lax.rem(par, 2), par // 2
    near = side * 2 + (1 - core)
    across = (1 - side) * 2 + core
    corner = (1 - side) * 2 + (1 - core)
    bins_dev, sensors, params = real_v.shape
    count = probes_v.shape[0]
    pending = []

    def send(src, dst, send_sem, recv_sem, par_to, freq_to):
        copy = pltpu.make_async_remote_copy(
            src_ref=src, dst_ref=dst, send_sem=send_sem, recv_sem=recv_sem,
            device_id=(par_to, freq_to), device_id_type=MESH,
        )
        copy.start()
        pending.append(copy)

    def arrived(dst, sem):
        pltpu.make_async_remote_copy(
            src_ref=dst, dst_ref=dst, send_sem=sem, recv_sem=sem,
            device_id=(near, freq), device_id_type=MESH,
        ).wait_recv()

    loads = [pltpu.make_async_copy(probes_hbm.at[r], probes_v.at[r], load_sem.at[r]) for r in range(count)]
    for copy in loads:
        copy.start()
    maps = [
        pltpu.make_async_copy(real_hbm, real_v, map_sem.at[0]),
        pltpu.make_async_copy(imag_hbm, imag_v, map_sem.at[1]),
    ]
    for copy in maps:
        copy.start()

    barrier = pltpu.get_barrier_semaphore()
    for d in range(1, freq_count):
        pl.semaphore_signal(
            barrier, inc=1, device_id=(par, lax.rem(freq + d, freq_count)), device_id_type=MESH
        )
    for other in (near, across):
        pl.semaphore_signal(barrier, inc=1, device_id=(other, freq), device_id_type=MESH)

    o_buf[...] = jnp.zeros_like(o_buf)
    w_buf[...] = jnp.zeros_like(w_buf)
    t_own[...] = jnp.zeros_like(t_own)
    table = table_ref[par]
    for r in range(count):
        loads[r].wait()
        rows = lax.dot_general(table, probes_v[r], (((1,), (1,)), ((), ())), preferred_element_type=F32)
        o_buf[:, r, :, 0:sensors] = rows.astype(BF16).reshape(STAGES, ROWS, sensors)
    width = o_buf.shape[-1]
    swap = swap_ref[...]

    def spread(i):
        mixed = o_buf[i].reshape(count * ROWS, width)
        mixed = jnp.dot(swap, mixed, preferred_element_type=F32).astype(BF16)
        s_buf[i] = mixed.reshape(freq_count, ROWS, width)
        v_buf[STAGES * par + i, freq] = s_buf[i, freq]

    def send_spectra(i):
        for d in range(1, freq_count):
            to = lax.rem(freq + d, freq_count)
            send(s_buf.at[i, to], v_buf.at[STAGES * par + i, freq], f_send.at[i, to], f_recv.at[i, freq], par, to)

    def gather(i):
        for d in range(1, freq_count):
            src = lax.rem(freq + freq_count - d, freq_count)
            arrived(v_buf.at[STAGES * par + i, src], f_recv.at[i, src])
        block = v_buf.at[STAGES * par + i]
        send(block, block, g_send.at[i, 0], g_recv.at[i, 0], across, freq)
        send(block, block, g_send.at[i, 1], g_recv.at[i, 1], near, freq)

    def gather_on(i):
        block = v_buf.at[STAGES * across + i]
        arrived(block, g_recv.at[i, 0])
        send(block, block, h_send.at[i], h_recv.at[i], near, freq)

    prior = prior_ref[...]

    def compute(i):
        arrived(v_buf.at[STAGES * near + i], g_recv.at[i, 1])
        arrived(v_buf.at[STAGES * corner + i], h_recv.at[i])
        if i == 0:
            for copy in maps:
                copy.wait()

        def one(member, carry):
            bin_at = STAGES * member + i

            @pl.when(bin_at < bins_dev)
            def _():
                real, imag = real_v[bin_at], imag_v[bin_at]
                v = v_buf[bin_at].reshape(freq_count * ROWS, width)[:, :sensors]
                left = jnp.dot(v, real, preferred_element_type=F32).reshape(freq_count, 2, count, params)
                right = jnp.dot(v, imag, preferred_element_type=F32).reshape(freq_count, 2, count, params)
                u_real = left[:, 0] + right[:, 1]
                u_imag = left[:, 1] - right[:, 0]
                weight = jnp.where(freq * bins_dev + bin_at == 0, 1.0, 2.0).astype(F32)
                t_own[...] += weight * prior * jnp.sum(u_real * u_real + u_imag * u_imag, axis=0)
                scaled = jnp.stack([u_real * prior, u_imag * prior], axis=1)
                scaled = scaled.reshape(freq_count * ROWS, params).astype(BF16)
                turn = (((1,), (1,)), ((), ()))
                left = lax.dot_general(scaled, real, turn, preferred_element_type=F32)
                right = lax.dot_general(scaled, imag, turn, preferred_element_type=F32)
                left = left.reshape(freq_count, 2, count, sensors)
                right = right.reshape(freq_count, 2, count, sensors)
                w = jnp.stack([left[:, 0] - right[:, 1], left[:, 1] + right[:, 0]], axis=1)
                w_buf[bin_at, :, :, 0:sensors] = w.reshape(freq_count, ROWS, sensors).astype(BF16)

            return carry

        lax.fori_loop(0, 4, one, 0)
        for s in range(2):
            send(
                w_buf.at[STAGES * (2 * s + 1 - core) + i], a_buf.at[s, i],
                r_send.at[i, s], r_recv.at[i, s], near, freq,
            )

    def reduce_core(i):
        for s in range(2):
            arrived(a_buf.at[s, i], r_recv.at[i, s])
        total = w_buf[STAGES * across + i].astype(F32) + a_buf[1 - side, i].astype(F32)
        h_buf[i] = total.astype(BF16)
        send(h_buf.at[i], b_buf.at[i], rx_send.at[i], rx_recv.at[i], across, freq)

    def reduce_across(i):
        arrived(b_buf.at[i], rx_recv.at[i])
        total = w_buf[STAGES * par + i].astype(F32) + a_buf[side, i].astype(F32) + b_buf[i].astype(F32)
        q_buf[i] = total.astype(BF16)
        y_buf[freq, STAGES * par + i] = q_buf[i, freq]
        for d in range(1, freq_count):
            to = lax.rem(freq + d, freq_count)
            send(q_buf.at[i, to], y_buf.at[freq, STAGES * par + i], bf_send.at[i, to], bf_recv.at[i, freq], par, to)

    def back(i):
        for d in range(1, freq_count):
            src = lax.rem(freq + freq_count - d, freq_count)
            arrived(y_buf.at[src, STAGES * par + i], bf_recv.at[i, src])
        block = y_buf.at[:, STAGES * par + i]
        send(block, block, bg_send.at[i, 0], bg_recv.at[i, 0], across, freq)
        send(block, block, bg_send.at[i, 1], bg_recv.at[i, 1], near, freq)

    def back_on(i):
        block = y_buf.at[:, STAGES * across + i]
        arrived(block, bg_recv.at[i, 0])
        send(block, block, bh_send.at[i], bh_recv.at[i], near, freq)

    def finish(i):
        arrived(y_buf.at[:, STAGES * near + i], bg_recv.at[i, 1])
        arrived(y_buf.at[:, STAGES * corner + i], bh_recv.at[i])

    def trace_freq():
        t_freq[freq] = t_own[...]
        for d in range(1, freq_count):
            to = lax.rem(freq + d, freq_count)
            send(t_own, t_freq.at[freq], t_send.at[to], t_recv.at[freq], par, to)

    def trace_core():
        for d in range(1, freq_count):
            src = lax.rem(freq + freq_count - d, freq_count)
            arrived(t_freq.at[src], t_recv.at[src])
        t_mid[...] = jnp.sum(t_freq[...], axis=0)
        send(t_mid, t_core, tp_send.at[0], tp_recv.at[0], near, freq)

    def trace_across():
        arrived(t_core, tp_recv.at[0])
        t_half[...] = t_mid[...] + t_core[...]
        send(t_half, t_x, tp_send.at[1], tp_recv.at[1], across, freq)

    spread(0)
    pl.semaphore_wait(barrier, freq_count + 1)
    send_spectra(0)
    for i in range(1, STAGES):
        spread(i)
        send_spectra(i)
    gather(0)
    gather(1)
    gather_on(0)
    compute(0)
    gather(2)
    gather_on(1)
    reduce_core(0)
    compute(1)
    gather(3)
    gather_on(2)
    reduce_core(1)
    compute(2)
    gather_on(3)
    reduce_core(2)
    reduce_across(0)
    compute(3)
    trace_freq()
    reduce_core(3)
    reduce_across(1)
    trace_core()
    back(0)
    reduce_across(2)
    trace_across()
    back_on(0)
    reduce_across(3)
    back(1)
    back_on(1)
    back(2)
    back_on(2)
    back(3)
    back_on(3)
    for i in range(STAGES):
        finish(i)
    arrived(t_x, tp_recv.at[1])
    trace_ref[...] = t_half[...] + t_x[...]
    out = pltpu.make_async_copy(y_buf, y_hbm, out_sem)
    out.start()
    for copy in pending:
        copy.wait_send()
    out.wait()


def inverse_kernel(factor, y_ref, trace_ref, swap_ref, table_ref, probes_ref, out_ref, x_buf):
    at = pl.program_id(0)
    freq_count, padded, rows, width = y_ref.shape
    count = rows // 2
    sensors = out_ref.shape[1]

    @pl.when(at == 0)
    def _():
        swap = swap_ref[...]
        for g in range(freq_count):
            for h in range(padded // 8):
                block = y_ref[g, 8 * h : 8 * h + 8].reshape(8 * rows, width)
                block = jnp.dot(swap, block, preferred_element_type=F32).astype(BF16)
                x_buf[:, g * (padded // 8) + h] = block.reshape(count, rows, width)

    trace_est = jnp.sum(trace_ref[...]) * factor
    block = x_buf[at].reshape(freq_count * padded * 2, width)
    response = lax.dot_general(block, table_ref[...], (((0,), (0,)), ((), ())), preferred_element_type=F32)
    response = response[:sensors]
    out_ref[0] = (response + trace_est * probes_ref[0].astype(F32)).astype(BF16)


def fast_shards(probes, map_real, map_imag, prior_var):
    freq_count, par_count = lax.axis_size("freq"), lax.axis_size("par")
    bins_dev, sensors, params = map_real.shape
    count, _, steps = probes.shape
    padded = STAGES * par_count
    width = -(-sensors // 128) * 128
    forward, inverse = tables(steps, bins_dev, freq_count, par_count)
    forward, inverse = jnp.asarray(forward, BF16), jnp.asarray(inverse, BF16)
    swap_out = jnp.asarray(swap_matrix(count, ROWS), BF16)
    swap_in = jnp.asarray(swap_matrix(ROWS, count), BF16)
    vmem, any_place = pl.BlockSpec(memory_space=pltpu.VMEM), pl.BlockSpec(memory_space=pl.ANY)
    dma = pltpu.SemaphoreType.DMA
    block = (freq_count, ROWS, width)
    small = pltpu.VMEM((count, params), F32)
    y, trace = pl.pallas_call(
        functools.partial(exchange_kernel, freq_count),
        out_shape=(
            jax.ShapeDtypeStruct((freq_count, padded, ROWS, width), BF16),
            jax.ShapeDtypeStruct((count, params), F32),
        ),
        in_specs=[vmem, vmem, vmem, any_place, any_place, any_place],
        out_specs=(any_place, vmem),
        scratch_shapes=[
            pltpu.VMEM(probes.shape, BF16),
            pltpu.VMEM(map_real.shape, BF16),
            pltpu.VMEM(map_imag.shape, BF16),
            pltpu.VMEM((STAGES, count, ROWS, width), BF16),
            pltpu.VMEM((STAGES,) + block, BF16),
            pltpu.VMEM((padded,) + block, BF16),
            pltpu.VMEM((padded,) + block, BF16),
            pltpu.VMEM((2, STAGES) + block, BF16),
            pltpu.VMEM((STAGES,) + block, BF16),
            pltpu.VMEM((STAGES,) + block, BF16),
            pltpu.VMEM((STAGES,) + block, BF16),
            pltpu.VMEM((freq_count, padded, ROWS, width), BF16),
            small,
            pltpu.VMEM((freq_count, count, params), F32),
            small,
            small,
            small,
            small,
            dma((count,)),
            dma((2,)),
            dma,
            dma((STAGES, freq_count)),
            dma((STAGES, freq_count)),
            dma((STAGES, 2)),
            dma((STAGES, 2)),
            dma((STAGES,)),
            dma((STAGES,)),
            dma((STAGES, 2)),
            dma((STAGES, 2)),
            dma((STAGES,)),
            dma((STAGES,)),
            dma((STAGES, freq_count)),
            dma((STAGES, freq_count)),
            dma((STAGES, 2)),
            dma((STAGES, 2)),
            dma((STAGES,)),
            dma((STAGES,)),
            dma((freq_count,)),
            dma((freq_count,)),
            dma((2,)),
            dma((2,)),
        ],
        compiler_params=pltpu.CompilerParams(
            collective_id=0, has_side_effects=True, vmem_limit_bytes=60 * 1024 * 1024
        ),
        name="exchange",
    )(forward, swap_out, prior_var.reshape(1, params), probes, map_real, map_imag)
    factor = noise_ratio / (count * freq_count * sensors * steps)
    return pl.pallas_call(
        functools.partial(inverse_kernel, factor),
        grid=(count,),
        out_shape=jax.ShapeDtypeStruct(probes.shape, BF16),
        in_specs=[
            pl.BlockSpec(y.shape, lambda r: (0, 0, 0, 0)),
            pl.BlockSpec(trace.shape, lambda r: (0, 0)),
            pl.BlockSpec(swap_in.shape, lambda r: (0, 0)),
            pl.BlockSpec(inverse.shape, lambda r: (0, 0)),
            pl.BlockSpec((1, sensors, steps), lambda r: (r, 0, 0)),
        ],
        out_specs=pl.BlockSpec((1, sensors, steps), lambda r: (r, 0, 0)),
        scratch_shapes=[pltpu.VMEM((count, freq_count * padded // 8, ROWS, width), BF16)],
        compiler_params=pltpu.CompilerParams(vmem_limit_bytes=48 * 1024 * 1024),
        name="inverse",
    )(y, trace, swap_in, inverse, probes)


def shards(probes, map_real, map_imag, prior_var):
    fits = lax.axis_size("par") == 4 and lax.axis_size("freq") == 8
    fits = fits and probes.shape[0] == 8 and map_real.shape[0] <= 16
    return (fast_shards if fits else plain_shards)(probes, map_real, map_imag, prior_var)


def solution(mesh):
    placed = (P("freq", None, None), P("freq", None, "par"), P("freq", None, "par"), P("par"))
    return jax.shard_map(
        shards, mesh=mesh, in_specs=placed, out_specs=P("freq", None, None), check_vma=False
    )
```

```python
import functools

import jax
import jax.numpy as jnp
import numpy as np
from jax import lax
from jax.experimental import pallas as pl
from jax.experimental.pallas import tpu as pltpu
from jax.sharding import PartitionSpec as P

SENSORS = 600
STEPS = 420
PERIOD = 840
PROBES = 64


noise_ratio = 0.5


def split_product(left, table):
    upper = table.astype(jnp.bfloat16)
    lower = (table - upper.astype(jnp.float32)).astype(jnp.bfloat16)
    return jnp.dot(left, upper, preferred_element_type=jnp.float32) + jnp.dot(
        left, lower, preferred_element_type=jnp.float32
    )


def plain_shards(probes, map_real, map_imag, prior_var):
    freq_count = lax.axis_size("freq")
    bins_dev = map_real.shape[0]
    probe_block = probes.shape[0]
    total_bins = bins_dev * freq_count
    time_steps = jnp.arange(STEPS, dtype=jnp.int32)
    bin_index = jnp.arange(total_bins, dtype=jnp.int32)
    product_index = time_steps[:, None] * bin_index[None, :] % PERIOD
    angles = product_index.astype(jnp.float32) * (2.0 * jnp.pi / PERIOD)
    norm_scale = 1.0 / jnp.sqrt(jnp.float32(PERIOD))
    cosines = jnp.cos(angles) * norm_scale
    sines = jnp.sin(angles) * norm_scale
    forward = jnp.stack([cosines, -sines], axis=2).reshape(STEPS, 2 * total_bins)
    all_weight = jnp.where(bin_index == 0, 1.0, 2.0).astype(jnp.float32)
    inverse = jnp.stack([cosines * all_weight[None, :], -sines * all_weight[None, :]], axis=2)
    inverse = inverse.reshape(STEPS, 2 * total_bins).T
    flattened = probes.reshape(probe_block * SENSORS, STEPS)
    spectrum = split_product(flattened, forward).astype(jnp.bfloat16)
    spectrum = spectrum.reshape(probe_block, SENSORS, 2 * total_bins)
    exchanged = lax.all_to_all(spectrum, "freq", split_axis=2, concat_axis=0, tiled=True)
    all_probes = exchanged.shape[0]
    operand = exchanged.reshape(all_probes, SENSORS, bins_dev, 2).transpose(2, 1, 3, 0)
    operand = operand.reshape(bins_dev, SENSORS, 2 * all_probes)
    left_real = jnp.einsum("ksp,ksc->kpc", map_real, operand, preferred_element_type=jnp.float32)
    left_imag = jnp.einsum("ksp,ksc->kpc", map_imag, operand, preferred_element_type=jnp.float32)
    u_real = left_real[..., :all_probes] + left_imag[..., all_probes:]
    u_imag = left_real[..., all_probes:] - left_imag[..., :all_probes]
    global_bin = lax.axis_index("freq") * bins_dev + jnp.arange(bins_dev, dtype=jnp.int32)
    bin_weight = jnp.where(global_bin == 0, 1.0, 2.0).astype(jnp.float32)
    quadratic = jnp.sum(
        bin_weight[:, None, None] * prior_var[None, :, None] * (u_real * u_real + u_imag * u_imag)
    )
    trace_est = lax.psum(quadratic, ("par", "freq")) / (PROBES * SENSORS * STEPS)
    scaled = (jnp.concatenate([u_real, u_imag], axis=-1) * prior_var[None, :, None]).astype(
        jnp.bfloat16
    )
    right_real = jnp.einsum("ksp,kpc->ksc", map_real, scaled, preferred_element_type=jnp.float32)
    right_imag = jnp.einsum("ksp,kpc->ksc", map_imag, scaled, preferred_element_type=jnp.float32)
    w_partial = jnp.concatenate(
        [
            right_real[..., :all_probes] - right_imag[..., all_probes:],
            right_real[..., all_probes:] + right_imag[..., :all_probes],
        ],
        axis=-1,
    )
    summed = lax.psum(w_partial.astype(jnp.bfloat16), "par")
    outgoing = summed.reshape(bins_dev, SENSORS, 2, all_probes).transpose(3, 1, 0, 2)
    outgoing = outgoing.reshape(all_probes, SENSORS, 2 * bins_dev)
    by_probe = lax.all_to_all(outgoing, "freq", split_axis=0, concat_axis=2, tiled=True)
    by_rows = by_probe.reshape(probe_block * SENSORS, 2 * total_bins)
    response = split_product(by_rows, inverse).reshape(probe_block, SENSORS, STEPS)
    return (response + noise_ratio * trace_est * probes.astype(jnp.float32)).astype(jnp.bfloat16)


MESH = pl.DeviceIdType.MESH
ROWS = 16
GROUP = 4
F32, BF16 = jnp.float32, jnp.bfloat16


def stage_members(stage, bins_dev):
    return (0, 1, 2, 3) if bins_dev - GROUP * stage >= GROUP else (0, 3)


def tables(steps, bins_dev, freq_count):
    stages = -(-bins_dev // GROUP)
    bins = np.arange(freq_count * bins_dev)
    angle = 2.0 * np.pi * ((bins[:, None] * np.arange(steps)) % PERIOD) / PERIOD
    both = np.stack([np.cos(angle), -np.sin(angle)], axis=1) / np.sqrt(PERIOD)
    weighted = both * np.where(bins == 0, 1.0, 2.0)[:, None, None]
    both = both.reshape(freq_count, bins_dev, 2, steps)
    weighted = weighted.reshape(freq_count, bins_dev, 2, steps)
    forward = np.zeros((GROUP, stages, freq_count, 2, steps))
    inverse = []
    for stage in range(stages):
        members = stage_members(stage, bins_dev)
        for n, member in enumerate(members):
            forward[member, stage] = both[:, GROUP * stage + n]
        inverse.append(weighted[:, GROUP * stage : GROUP * stage + len(members)].reshape(-1, steps))
    forward = forward.reshape(GROUP, stages * freq_count * 2, steps)
    return forward.astype(np.float32), np.concatenate(inverse).astype(np.float32)


def swap_matrix(outer, inner):
    out = np.arange(outer * inner)
    matrix = np.zeros((out.size, out.size), np.float32)
    matrix[out, (out % outer) * inner + out // outer] = 1.0
    return matrix


def exchange_kernel(
    freq_count, table_ref, swap_ref, back_ref, prior_ref, probes_hbm, real_hbm, imag_hbm, x_hbm, trace_ref,
    probes_v, split_v, real_v, imag_v, o_buf, s_buf, v_buf, w_buf, a_buf, h_buf, b_buf, q_buf, y_buf, x_buf,
    t_own, t_freq, t_mid, t_core, t_half, t_x,
    load_sem, map_sem, out_sem, f_send, f_recv, g_send, g_recv, h_send, h_recv,
    r_send, r_recv, rx_send, rx_recv, bf_send, bf_recv, bg_send, bg_recv, bh_send, bh_recv,
    t_send, t_recv, tp_send, tp_recv,
):
    par, freq = lax.axis_index("par"), lax.axis_index("freq")
    core, side = lax.rem(par, 2), par // 2
    near = side * 2 + (1 - core)
    across = (1 - side) * 2 + core
    corner = (1 - side) * 2 + (1 - core)
    bins_dev, sensors, params = real_v.shape
    steps, count = probes_v.shape[:2]
    stages, width = o_buf.shape[0], o_buf.shape[-1]
    lanes = [(128 * j, min(128, sensors - 128 * j)) for j in range(width // 128)]
    outer = core == side
    inner = core != side
    pending = []

    def when(i, condition, body):
        if len(stage_members(i, bins_dev)) == GROUP:
            body()
        else:
            pl.when(condition)(body)

    def send(i, condition, make):
        make().start()
        pending.append((i, condition, make))

    def remote(src, dst, send_sem, recv_sem, par_to, freq_to):
        return pltpu.make_async_remote_copy(
            src_ref=src, dst_ref=dst, send_sem=send_sem, recv_sem=recv_sem,
            device_id=(par_to, freq_to), device_id_type=MESH,
        )

    def arrived(dst, sem):
        remote(dst, dst, sem, sem, near, freq).wait_recv()

    pieces = load_sem.shape[0]
    piece = steps // pieces
    loads = [
        pltpu.make_async_copy(
            probes_hbm.at[pl.ds(n * piece, piece)], probes_v.at[pl.ds(n * piece, piece)], load_sem.at[n]
        )
        for n in range(pieces)
    ]
    for copy in loads:
        copy.start()
    maps = [
        pltpu.make_async_copy(real_hbm, real_v, map_sem.at[0]),
        pltpu.make_async_copy(imag_hbm, imag_v, map_sem.at[1]),
    ]
    for copy in maps:
        copy.start()

    def peer(d):
        return lax.rem(freq + d, freq_count)

    barrier = pltpu.get_barrier_semaphore()
    for d in range(1, freq_count):
        pl.semaphore_signal(barrier, inc=1, device_id=(par, peer(d)), device_id_type=MESH)
    for other in (near, across):
        pl.semaphore_signal(barrier, inc=1, device_id=(other, freq), device_id_type=MESH)

    o_buf[...] = jnp.zeros_like(o_buf)
    w_buf[...] = jnp.zeros_like(w_buf)
    t_own[...] = jnp.zeros_like(t_own)
    split_v[len(lanes) - 1] = jnp.zeros_like(split_v[len(lanes) - 1])
    for n in range(pieces):
        loads[n].wait()
        rows = probes_v[n * piece : (n + 1) * piece].astype(F32).reshape(piece * count, sensors)
        for j, (start, size) in enumerate(lanes):
            split_v[j, n * piece * count : (n + 1) * piece * count, 0:size] = rows[:, start : start + size]
    table = table_ref[par]
    for r in range(count):
        one = [split_v[j, pl.ds(r, steps, stride=count), :].astype(BF16) for j in range(len(lanes))]
        rows = jnp.dot(table, jnp.concatenate(one, axis=1), preferred_element_type=F32)
        o_buf[:, r] = rows.astype(BF16).reshape(stages, ROWS, width)
    swap = swap_ref[...]

    def spread(i):
        mixed = o_buf[i].reshape(count * ROWS, width)
        mixed = jnp.dot(swap, mixed, preferred_element_type=F32).astype(BF16)
        s_buf[i] = mixed.reshape(freq_count, ROWS, width)
        v_buf[stages * par + i, freq] = s_buf[i, freq]

    def send_spectra(i):
        def body():
            for d in range(1, freq_count):
                send(i, outer, lambda d=d: remote(
                    s_buf.at[i, peer(d)], v_buf.at[stages * par + i, freq],
                    f_send.at[i, peer(d)], f_recv.at[i, freq], par, peer(d),
                ))

        when(i, outer, body)

    def gather(i):
        def body():
            for d in range(1, freq_count):
                src = peer(freq_count - d)
                arrived(v_buf.at[stages * par + i, src], f_recv.at[i, src])
            for k, to in enumerate((across, near)):
                send(i, outer, lambda k=k, to=to: remote(
                    v_buf.at[stages * par + i], v_buf.at[stages * par + i],
                    g_send.at[i, k], g_recv.at[i, k], to, freq,
                ))

        when(i, outer, body)

    def gather_on(i):
        def body():
            arrived(v_buf.at[stages * across + i], g_recv.at[i, 0])
            send(i, inner, lambda: remote(
                v_buf.at[stages * across + i], v_buf.at[stages * across + i],
                h_send.at[i], h_recv.at[i], near, freq,
            ))

        when(i, inner, body)

    prior = prior_ref[...]

    def compute(i):
        members = stage_members(i, bins_dev)
        when(i, inner, lambda: arrived(v_buf.at[stages * near + i], g_recv.at[i, 1]))
        when(i, outer, lambda: arrived(v_buf.at[stages * corner + i], h_recv.at[i]))
        if i == 0:
            for copy in maps:
                copy.wait()

        def one(n, carry):
            slot = stages * n * ((GROUP - 1) // (len(members) - 1)) + i
            bin_at = GROUP * i + n
            real, imag = real_v[bin_at], imag_v[bin_at]
            v = v_buf[slot].reshape(freq_count * ROWS, width)[:, :sensors]
            left = jnp.dot(v, real, preferred_element_type=F32).reshape(freq_count, 2, count, params)
            right = jnp.dot(v, imag, preferred_element_type=F32).reshape(freq_count, 2, count, params)
            u_real = left[:, 0] + right[:, 1]
            u_imag = left[:, 1] - right[:, 0]
            weight = jnp.where(freq * bins_dev + bin_at == 0, 1.0, 2.0).astype(F32)
            t_own[...] += weight * prior * jnp.sum(u_real * u_real + u_imag * u_imag, axis=0)
            scaled = jnp.stack([u_real * prior, u_imag * prior], axis=1)
            scaled = scaled.reshape(freq_count * ROWS, params).astype(BF16)
            turn = (((1,), (1,)), ((), ()))
            left = lax.dot_general(scaled, real, turn, preferred_element_type=F32)
            right = lax.dot_general(scaled, imag, turn, preferred_element_type=F32)
            left = left.reshape(freq_count, 2, count, sensors)
            right = right.reshape(freq_count, 2, count, sensors)
            w = jnp.stack([left[:, 0] - right[:, 1], left[:, 1] + right[:, 0]], axis=1)
            w_buf[slot, :, :, 0:sensors] = w.reshape(freq_count, ROWS, sensors).astype(BF16)
            return carry

        lax.fori_loop(0, len(members), one, 0)

        def give(owner, owner_side, condition):
            def body():
                send(i, condition, lambda: remote(
                    w_buf.at[stages * owner + i], a_buf.at[owner_side, i],
                    r_send.at[i, owner_side], r_recv.at[i, owner_side], near, freq,
                ))

            when(i, condition, body)

        give(corner, 1 - side, outer)
        give(near, side, inner)

    def reduce_core(i):
        def body():
            arrived(a_buf.at[1 - side, i], r_recv.at[i, 1 - side])
            total = w_buf[stages * across + i].astype(F32) + a_buf[1 - side, i].astype(F32)
            h_buf[i] = total.astype(BF16)
            send(i, inner, lambda: remote(h_buf.at[i], b_buf.at[i], rx_send.at[i], rx_recv.at[i], across, freq))

        when(i, inner, body)

    def reduce_across(i):
        def body():
            arrived(a_buf.at[side, i], r_recv.at[i, side])
            arrived(b_buf.at[i], rx_recv.at[i])
            total = w_buf[stages * par + i].astype(F32) + a_buf[side, i].astype(F32) + b_buf[i].astype(F32)
            q_buf[i] = total.astype(BF16)
            y_buf[freq, stages * par + i] = q_buf[i, freq]
            for d in range(1, freq_count):
                send(i, outer, lambda d=d: remote(
                    q_buf.at[i, peer(d)], y_buf.at[freq, stages * par + i],
                    bf_send.at[i, peer(d)], bf_recv.at[i, freq], par, peer(d),
                ))

        when(i, outer, body)

    def back(i):
        def body():
            for d in range(1, freq_count):
                src = peer(freq_count - d)
                arrived(y_buf.at[src, stages * par + i], bf_recv.at[i, src])
            for k, to in enumerate((across, near)):
                send(i, outer, lambda k=k, to=to: remote(
                    y_buf.at[:, stages * par + i], y_buf.at[:, stages * par + i],
                    bg_send.at[i, k], bg_recv.at[i, k], to, freq,
                ))

        when(i, outer, body)

    def back_on(i):
        def body():
            arrived(y_buf.at[:, stages * across + i], bg_recv.at[i, 0])
            send(i, inner, lambda: remote(
                y_buf.at[:, stages * across + i], y_buf.at[:, stages * across + i],
                bh_send.at[i], bh_recv.at[i], near, freq,
            ))

        when(i, inner, body)

    turn_back = back_ref[...]
    outs = []

    def finish(i):
        when(i, inner, lambda: arrived(y_buf.at[:, stages * near + i], bg_recv.at[i, 1]))
        when(i, outer, lambda: arrived(y_buf.at[:, stages * corner + i], bh_recv.at[i]))
        members = stage_members(i, bins_dev)
        slabs = [(g, stages * m + i) for g in range(freq_count) for m in members]
        first = GROUP * i * freq_count // 8
        for b in range(len(slabs) // 8):
            block = jnp.concatenate([y_buf[g, slot] for g, slot in slabs[8 * b : 8 * b + 8]], axis=0)
            block = jnp.dot(turn_back, block, preferred_element_type=F32).astype(BF16)
            x_buf[:, first + b] = block.reshape(count, ROWS, width)
        part = pl.ds(first, len(slabs) // 8)
        outs.append(pltpu.make_async_copy(x_buf.at[:, part], x_hbm.at[:, part], out_sem.at[i]))
        outs[-1].start()

    def trace_freq():
        t_freq[freq] = t_own[...]
        for d in range(1, freq_count):
            send(0, None, lambda d=d: remote(
                t_own, t_freq.at[freq], t_send.at[peer(d)], t_recv.at[freq], par, peer(d)
            ))

    def trace_core():
        for d in range(1, freq_count):
            src = peer(freq_count - d)
            arrived(t_freq.at[src], t_recv.at[src])
        t_mid[...] = jnp.sum(t_freq[...], axis=0)
        send(0, None, lambda: remote(t_mid, t_core, tp_send.at[0], tp_recv.at[0], near, freq))

    def trace_across():
        arrived(t_core, tp_recv.at[0])
        t_half[...] = t_mid[...] + t_core[...]
        send(0, None, lambda: remote(t_half, t_x, tp_send.at[1], tp_recv.at[1], across, freq))

    last = stages - 1
    spread(0)
    pl.semaphore_wait(barrier, freq_count + 1)
    send_spectra(0)
    for i in range(1, stages):
        spread(i)
        send_spectra(i)
    gather(0)
    for i in range(stages):
        if i < last:
            gather(i + 1)
        gather_on(i)
        if i > 0:
            reduce_core(i - 1)
        if i > 2:
            reduce_across(i - 3)
        compute(i)
    trace_freq()
    reduce_core(last)
    for i in range(max(last - 2, 0), last):
        reduce_across(i)
    trace_core()
    back(0)
    reduce_across(last)
    trace_across()
    back_on(0)
    for i in range(1, stages):
        back(i)
        finish(i - 1)
        back_on(i)
    finish(last)
    arrived(t_x, tp_recv.at[1])
    trace_ref[...] = t_half[...] + t_x[...]
    for i, condition, make in pending:
        when(i, condition, lambda make=make: make().wait_send())
    for copy in outs:
        copy.wait()


def inverse_kernel(factor, x_ref, trace_ref, table_ref, probes_ref, out_ref, split_v):
    count, blocks, rows, width = x_ref.shape
    piece, _, sensors = out_ref.shape
    table = table_ref[0]
    trace_est = jnp.sum(trace_ref[...]) * factor
    for r in range(count):
        block = x_ref[r].reshape(blocks * rows, width)
        response = jnp.dot(table, block, preferred_element_type=F32)
        for j in range(width // 128):
            split_v[j, pl.ds(r, piece, stride=count), :] = response[:, 128 * j : 128 * j + 128]
    for j in range(width // 128):
        start, size = 128 * j, min(128, sensors - 128 * j)
        part = split_v[j].reshape(piece, count, 128)[:, :, :size]
        noise = trace_est * probes_ref[:, :, start : start + size].astype(F32)
        out_ref[:, :, start : start + size] = (part + noise).astype(BF16)


def fast_shards(probes, map_real, map_imag, prior_var):
    freq_count = lax.axis_size("freq")
    bins_dev, sensors, params = map_real.shape
    count, _, steps = probes.shape
    stages = -(-bins_dev // GROUP)
    padded = stages * GROUP
    width = -(-sensors // 128) * 128
    pieces = next(n for n in (3, 4, 5, 2, 1) if steps % n == 0)
    forward, inverse = tables(steps, bins_dev, freq_count)
    blocks = inverse.shape[0] // ROWS
    inverse = jnp.asarray(inverse.T.reshape(pieces, steps // pieces, -1), BF16)
    forward = jnp.asarray(forward, BF16)
    swap_out = jnp.asarray(swap_matrix(count, ROWS), BF16)
    swap_in = jnp.asarray(swap_matrix(ROWS, count), BF16)
    by_time = probes.transpose(2, 0, 1)
    vmem, any_place = pl.BlockSpec(memory_space=pltpu.VMEM), pl.BlockSpec(memory_space=pl.ANY)
    dma = pltpu.SemaphoreType.DMA
    block = (freq_count, ROWS, width)
    small = pltpu.VMEM((count, params), F32)
    staged = pltpu.VMEM((stages,) + block, BF16)
    peers, pairs, single = dma((stages, freq_count)), dma((stages, 2)), dma((stages,))
    x, trace = pl.pallas_call(
        functools.partial(exchange_kernel, freq_count),
        out_shape=(
            jax.ShapeDtypeStruct((count, blocks, ROWS, width), BF16),
            jax.ShapeDtypeStruct((count, params), F32),
        ),
        in_specs=[vmem, vmem, vmem, vmem, any_place, any_place, any_place],
        out_specs=(any_place, vmem),
        scratch_shapes=[
            pltpu.VMEM(by_time.shape, BF16),
            pltpu.VMEM((width // 128, steps * count, 128), F32),
            pltpu.VMEM(map_real.shape, BF16),
            pltpu.VMEM(map_imag.shape, BF16),
            pltpu.VMEM((stages, count, ROWS, width), BF16),
            staged,
            pltpu.VMEM((padded,) + block, BF16),
            pltpu.VMEM((padded,) + block, BF16),
            pltpu.VMEM((2, stages) + block, BF16),
            staged,
            staged,
            staged,
            pltpu.VMEM((freq_count, padded, ROWS, width), BF16),
            pltpu.VMEM((count, blocks, ROWS, width), BF16),
            small,
            pltpu.VMEM((freq_count, count, params), F32),
            small,
            small,
            small,
            small,
            dma((pieces,)),
            dma((2,)),
            single,
            peers,
            peers,
            pairs,
            pairs,
            single,
            single,
            pairs,
            pairs,
            single,
            single,
            peers,
            peers,
            pairs,
            pairs,
            single,
            single,
            dma((freq_count,)),
            dma((freq_count,)),
            dma((2,)),
            dma((2,)),
        ],
        compiler_params=pltpu.CompilerParams(
            collective_id=0, has_side_effects=True, vmem_limit_bytes=60 * 1024 * 1024
        ),
        name="exchange",
    )(forward, swap_out, swap_in, prior_var.reshape(1, params), by_time, map_real, map_imag)
    factor = noise_ratio / (count * freq_count * sensors * steps)
    piece = steps // pieces
    result = pl.pallas_call(
        functools.partial(inverse_kernel, factor),
        grid=(pieces,),
        out_shape=jax.ShapeDtypeStruct(by_time.shape, BF16),
        in_specs=[
            pl.BlockSpec(x.shape, lambda n: (0, 0, 0, 0)),
            pl.BlockSpec(trace.shape, lambda n: (0, 0)),
            pl.BlockSpec((1, piece, blocks * ROWS), lambda n: (n, 0, 0)),
            pl.BlockSpec((piece, count, sensors), lambda n: (n, 0, 0)),
        ],
        out_specs=pl.BlockSpec((piece, count, sensors), lambda n: (n, 0, 0)),
        scratch_shapes=[pltpu.VMEM((width // 128, piece * count, 128), F32)],
        compiler_params=pltpu.CompilerParams(vmem_limit_bytes=48 * 1024 * 1024),
        name="inverse",
    )(x, trace, inverse, by_time)
    return result.transpose(1, 2, 0)


def shards(probes, map_real, map_imag, prior_var):
    fits = lax.axis_size("par") == GROUP and lax.axis_size("freq") == 8
    fits = fits and probes.shape[0] == 8 and map_real.shape[0] % 4 in (0, 2) and map_real.shape[0] > 8
    return (fast_shards if fits else plain_shards)(probes, map_real, map_imag, prior_var)


def solution(mesh):
    placed = (P("freq", None, None), P("freq", None, "par"), P("freq", None, "par"), P("par"))
    return jax.shard_map(
        shards, mesh=mesh, in_specs=placed, out_specs=P("freq", None, None), check_vma=False
    )
```

```python
import functools

import jax
import jax.numpy as jnp
import numpy as np
from jax import lax
from jax.experimental import pallas as pl
from jax.experimental.pallas import tpu as pltpu
from jax.sharding import PartitionSpec as P

SENSORS = 600
STEPS = 420
PERIOD = 840
PROBES = 64


noise_ratio = 0.5


def split_product(left, table):
    upper = table.astype(jnp.bfloat16)
    lower = (table - upper.astype(jnp.float32)).astype(jnp.bfloat16)
    return jnp.dot(left, upper, preferred_element_type=jnp.float32) + jnp.dot(
        left, lower, preferred_element_type=jnp.float32
    )


def plain_shards(probes, map_real, map_imag, prior_var):
    freq_count = lax.axis_size("freq")
    bins_dev = map_real.shape[0]
    probe_block = probes.shape[0]
    total_bins = bins_dev * freq_count
    time_steps = jnp.arange(STEPS, dtype=jnp.int32)
    bin_index = jnp.arange(total_bins, dtype=jnp.int32)
    product_index = time_steps[:, None] * bin_index[None, :] % PERIOD
    angles = product_index.astype(jnp.float32) * (2.0 * jnp.pi / PERIOD)
    norm_scale = 1.0 / jnp.sqrt(jnp.float32(PERIOD))
    cosines = jnp.cos(angles) * norm_scale
    sines = jnp.sin(angles) * norm_scale
    forward = jnp.stack([cosines, -sines], axis=2).reshape(STEPS, 2 * total_bins)
    all_weight = jnp.where(bin_index == 0, 1.0, 2.0).astype(jnp.float32)
    inverse = jnp.stack([cosines * all_weight[None, :], -sines * all_weight[None, :]], axis=2)
    inverse = inverse.reshape(STEPS, 2 * total_bins).T
    flattened = probes.reshape(probe_block * SENSORS, STEPS)
    spectrum = split_product(flattened, forward).astype(jnp.bfloat16)
    spectrum = spectrum.reshape(probe_block, SENSORS, 2 * total_bins)
    exchanged = lax.all_to_all(spectrum, "freq", split_axis=2, concat_axis=0, tiled=True)
    all_probes = exchanged.shape[0]
    operand = exchanged.reshape(all_probes, SENSORS, bins_dev, 2).transpose(2, 1, 3, 0)
    operand = operand.reshape(bins_dev, SENSORS, 2 * all_probes)
    left_real = jnp.einsum("ksp,ksc->kpc", map_real, operand, preferred_element_type=jnp.float32)
    left_imag = jnp.einsum("ksp,ksc->kpc", map_imag, operand, preferred_element_type=jnp.float32)
    u_real = left_real[..., :all_probes] + left_imag[..., all_probes:]
    u_imag = left_real[..., all_probes:] - left_imag[..., :all_probes]
    global_bin = lax.axis_index("freq") * bins_dev + jnp.arange(bins_dev, dtype=jnp.int32)
    bin_weight = jnp.where(global_bin == 0, 1.0, 2.0).astype(jnp.float32)
    quadratic = jnp.sum(
        bin_weight[:, None, None] * prior_var[None, :, None] * (u_real * u_real + u_imag * u_imag)
    )
    trace_est = lax.psum(quadratic, ("par", "freq")) / (PROBES * SENSORS * STEPS)
    scaled = (jnp.concatenate([u_real, u_imag], axis=-1) * prior_var[None, :, None]).astype(
        jnp.bfloat16
    )
    right_real = jnp.einsum("ksp,kpc->ksc", map_real, scaled, preferred_element_type=jnp.float32)
    right_imag = jnp.einsum("ksp,kpc->ksc", map_imag, scaled, preferred_element_type=jnp.float32)
    w_partial = jnp.concatenate(
        [
            right_real[..., :all_probes] - right_imag[..., all_probes:],
            right_real[..., all_probes:] + right_imag[..., :all_probes],
        ],
        axis=-1,
    )
    summed = lax.psum(w_partial.astype(jnp.bfloat16), "par")
    outgoing = summed.reshape(bins_dev, SENSORS, 2, all_probes).transpose(3, 1, 0, 2)
    outgoing = outgoing.reshape(all_probes, SENSORS, 2 * bins_dev)
    by_probe = lax.all_to_all(outgoing, "freq", split_axis=0, concat_axis=2, tiled=True)
    by_rows = by_probe.reshape(probe_block * SENSORS, 2 * total_bins)
    response = split_product(by_rows, inverse).reshape(probe_block, SENSORS, STEPS)
    return (response + noise_ratio * trace_est * probes.astype(jnp.float32)).astype(jnp.bfloat16)


MESH = pl.DeviceIdType.MESH
ROWS = 16
GROUP = 4
F32, BF16 = jnp.float32, jnp.bfloat16


def stage_members(stage, bins_dev):
    return (0, 1, 2, 3) if bins_dev - GROUP * stage >= GROUP else (0, 3)


def tables(steps, bins_dev, freq_count):
    stages = -(-bins_dev // GROUP)
    bins = np.arange(freq_count * bins_dev)
    angle = 2.0 * np.pi * ((bins[:, None] * np.arange(steps)) % PERIOD) / PERIOD
    both = np.stack([np.cos(angle), -np.sin(angle)], axis=1) / np.sqrt(PERIOD)
    weighted = both * np.where(bins == 0, 1.0, 2.0)[:, None, None]
    both = both.reshape(freq_count, bins_dev, 2, steps)
    weighted = weighted.reshape(freq_count, bins_dev, 2, steps)
    forward = np.zeros((GROUP, stages, freq_count, 2, steps))
    inverse = []
    for stage in range(stages):
        members = stage_members(stage, bins_dev)
        for n, member in enumerate(members):
            forward[member, stage] = both[:, GROUP * stage + n]
        inverse.append(weighted[:, GROUP * stage : GROUP * stage + len(members)].reshape(-1, steps))
    forward = forward.reshape(GROUP, stages * freq_count * 2, steps)
    return forward.astype(np.float32), np.concatenate(inverse).astype(np.float32)


def swap_matrix(outer, inner):
    out = np.arange(outer * inner)
    matrix = np.zeros((out.size, out.size), np.float32)
    matrix[out, (out % outer) * inner + out // outer] = 1.0
    return matrix


def exchange_kernel(
    freq_count, table_ref, swap_ref, back_ref, prior_ref, probes_hbm, real_hbm, imag_hbm, x_hbm, trace_ref,
    probes_v, split_v, real_v, imag_v, o_buf, s_buf, v_buf, w_buf, a_buf, h_buf, b_buf, q_buf, y_buf, x_buf,
    t_own, t_freq, t_mid, t_core, t_half, t_x,
    load_sem, map_sem, out_sem, f_send, f_recv, g_send, g_recv, h_send, h_recv,
    r_send, r_recv, rx_send, rx_recv, bf_send, bf_recv, bg_send, bg_recv, bh_send, bh_recv,
    t_send, t_recv, tp_send, tp_recv,
):
    par, freq = lax.axis_index("par"), lax.axis_index("freq")
    core, side = lax.rem(par, 2), par // 2
    near = side * 2 + (1 - core)
    across = (1 - side) * 2 + core
    corner = (1 - side) * 2 + (1 - core)
    bins_dev, sensors, params = real_v.shape
    steps, count = probes_v.shape[:2]
    stages, width = o_buf.shape[0], o_buf.shape[-1]
    lanes = [(128 * j, min(128, sensors - 128 * j)) for j in range(width // 128)]
    outer = core == side
    inner = core != side
    pending = []

    def when(i, condition, body):
        if len(stage_members(i, bins_dev)) == GROUP:
            body()
        else:
            pl.when(condition)(body)

    def send(i, condition, make):
        make().start()
        pending.append((i, condition, make))

    def remote(src, dst, send_sem, recv_sem, par_to, freq_to):
        return pltpu.make_async_remote_copy(
            src_ref=src, dst_ref=dst, send_sem=send_sem, recv_sem=recv_sem,
            device_id=(par_to, freq_to), device_id_type=MESH,
        )

    def arrived(dst, sem):
        remote(dst, dst, sem, sem, near, freq).wait_recv()

    pieces = load_sem.shape[0]
    piece = steps // pieces
    loads = [
        pltpu.make_async_copy(
            probes_hbm.at[pl.ds(n * piece, piece)], probes_v.at[pl.ds(n * piece, piece)], load_sem.at[n]
        )
        for n in range(pieces)
    ]
    for copy in loads:
        copy.start()
    maps = [
        pltpu.make_async_copy(real_hbm, real_v, map_sem.at[0]),
        pltpu.make_async_copy(imag_hbm, imag_v, map_sem.at[1]),
    ]

    def peer(d):
        return lax.rem(freq + d, freq_count)

    barrier = pltpu.get_barrier_semaphore()
    for d in range(1, freq_count):
        pl.semaphore_signal(barrier, inc=1, device_id=(par, peer(d)), device_id_type=MESH)
    for other in (near, across):
        pl.semaphore_signal(barrier, inc=1, device_id=(other, freq), device_id_type=MESH)

    o_buf[...] = jnp.zeros_like(o_buf)
    w_buf[...] = jnp.zeros_like(w_buf)
    t_own[...] = jnp.zeros_like(t_own)
    split_v[len(lanes) - 1] = jnp.zeros_like(split_v[len(lanes) - 1])
    for n in range(pieces):
        loads[n].wait()
        rows = probes_v[n * piece : (n + 1) * piece].astype(F32).reshape(piece * count, sensors)
        for j, (start, size) in enumerate(lanes):
            split_v[j, n * piece * count : (n + 1) * piece * count, 0:size] = rows[:, start : start + size]
    for copy in maps:
        copy.start()
    table = table_ref[par]
    for r in range(count):
        one = [split_v[j, pl.ds(r, steps, stride=count), :].astype(BF16) for j in range(len(lanes))]
        rows = jnp.dot(table, jnp.concatenate(one, axis=1), preferred_element_type=F32)
        o_buf[:, r] = rows.astype(BF16).reshape(stages, ROWS, width)
    swap = swap_ref[...]

    def spread(i):
        mixed = o_buf[i].reshape(count * ROWS, width)
        mixed = jnp.dot(swap, mixed, preferred_element_type=F32).astype(BF16)
        s_buf[i] = mixed.reshape(freq_count, ROWS, width)
        v_buf[stages * par + i, freq] = s_buf[i, freq]

    def send_spectra(i):
        def body():
            for d in range(1, freq_count):
                send(i, outer, lambda d=d: remote(
                    s_buf.at[i, peer(d)], v_buf.at[stages * par + i, freq],
                    f_send.at[i, peer(d)], f_recv.at[i, freq], par, peer(d),
                ))

        when(i, outer, body)

    def gather(i):
        def body():
            for d in range(1, freq_count):
                src = peer(freq_count - d)
                arrived(v_buf.at[stages * par + i, src], f_recv.at[i, src])
            for k, to in enumerate((across, near)):
                send(i, outer, lambda k=k, to=to: remote(
                    v_buf.at[stages * par + i], v_buf.at[stages * par + i],
                    g_send.at[i, k], g_recv.at[i, k], to, freq,
                ))

        when(i, outer, body)

    def gather_on(i):
        def body():
            arrived(v_buf.at[stages * across + i], g_recv.at[i, 0])
            send(i, inner, lambda: remote(
                v_buf.at[stages * across + i], v_buf.at[stages * across + i],
                h_send.at[i], h_recv.at[i], near, freq,
            ))

        when(i, inner, body)

    prior = prior_ref[...]

    def compute(i):
        members = stage_members(i, bins_dev)
        when(i, inner, lambda: arrived(v_buf.at[stages * near + i], g_recv.at[i, 1]))
        when(i, outer, lambda: arrived(v_buf.at[stages * corner + i], h_recv.at[i]))
        if i == 0:
            for copy in maps:
                copy.wait()

        def one(n, carry):
            slot = stages * n * ((GROUP - 1) // (len(members) - 1)) + i
            bin_at = GROUP * i + n
            real, imag = real_v[bin_at], imag_v[bin_at]
            v = v_buf[slot].reshape(freq_count * ROWS, width)[:, :sensors]
            left = jnp.dot(v, real, preferred_element_type=F32).reshape(freq_count, 2, count, params)
            right = jnp.dot(v, imag, preferred_element_type=F32).reshape(freq_count, 2, count, params)
            u_real = left[:, 0] + right[:, 1]
            u_imag = left[:, 1] - right[:, 0]
            weight = jnp.where(freq * bins_dev + bin_at == 0, 1.0, 2.0).astype(F32)
            t_own[...] += weight * prior * jnp.sum(u_real * u_real + u_imag * u_imag, axis=0)
            scaled = jnp.stack([u_real * prior, u_imag * prior], axis=1)
            scaled = scaled.reshape(freq_count * ROWS, params).astype(BF16)
            turn = (((1,), (1,)), ((), ()))
            left = lax.dot_general(scaled, real, turn, preferred_element_type=F32)
            right = lax.dot_general(scaled, imag, turn, preferred_element_type=F32)
            left = left.reshape(freq_count, 2, count, sensors)
            right = right.reshape(freq_count, 2, count, sensors)
            w = jnp.stack([left[:, 0] - right[:, 1], left[:, 1] + right[:, 0]], axis=1)
            w_buf[slot, :, :, 0:sensors] = w.reshape(freq_count, ROWS, sensors).astype(BF16)
            return carry

        lax.fori_loop(0, len(members), one, 0)

        def give(owner, owner_side, condition):
            def body():
                send(i, condition, lambda: remote(
                    w_buf.at[stages * owner + i], a_buf.at[owner_side, i],
                    r_send.at[i, owner_side], r_recv.at[i, owner_side], near, freq,
                ))

            when(i, condition, body)

        give(corner, 1 - side, outer)
        give(near, side, inner)

    def reduce_core(i):
        def body():
            arrived(a_buf.at[1 - side, i], r_recv.at[i, 1 - side])
            total = w_buf[stages * across + i].astype(F32) + a_buf[1 - side, i].astype(F32)
            h_buf[i] = total.astype(BF16)
            send(i, inner, lambda: remote(h_buf.at[i], b_buf.at[i], rx_send.at[i], rx_recv.at[i], across, freq))

        when(i, inner, body)

    def reduce_across(i):
        def body():
            arrived(a_buf.at[side, i], r_recv.at[i, side])
            arrived(b_buf.at[i], rx_recv.at[i])
            total = w_buf[stages * par + i].astype(F32) + a_buf[side, i].astype(F32) + b_buf[i].astype(F32)
            q_buf[i] = total.astype(BF16)
            y_buf[freq, stages * par + i] = q_buf[i, freq]
            for d in range(1, freq_count):
                send(i, outer, lambda d=d: remote(
                    q_buf.at[i, peer(d)], y_buf.at[freq, stages * par + i],
                    bf_send.at[i, peer(d)], bf_recv.at[i, freq], par, peer(d),
                ))

        when(i, outer, body)

    def back(i):
        def body():
            for d in range(1, freq_count):
                src = peer(freq_count - d)
                arrived(y_buf.at[src, stages * par + i], bf_recv.at[i, src])
            for k, to in enumerate((across, near)):
                send(i, outer, lambda k=k, to=to: remote(
                    y_buf.at[:, stages * par + i], y_buf.at[:, stages * par + i],
                    bg_send.at[i, k], bg_recv.at[i, k], to, freq,
                ))

        when(i, outer, body)

    def back_on(i):
        def body():
            arrived(y_buf.at[:, stages * across + i], bg_recv.at[i, 0])
            send(i, inner, lambda: remote(
                y_buf.at[:, stages * across + i], y_buf.at[:, stages * across + i],
                bh_send.at[i], bh_recv.at[i], near, freq,
            ))

        when(i, inner, body)

    turn_back = back_ref[...]
    outs = []

    def finish(i):
        when(i, inner, lambda: arrived(y_buf.at[:, stages * near + i], bg_recv.at[i, 1]))
        when(i, outer, lambda: arrived(y_buf.at[:, stages * corner + i], bh_recv.at[i]))
        members = stage_members(i, bins_dev)
        slabs = [(g, stages * m + i) for g in range(freq_count) for m in members]
        first = GROUP * i * freq_count // 8
        for b in range(len(slabs) // 8):
            block = jnp.concatenate([y_buf[g, slot] for g, slot in slabs[8 * b : 8 * b + 8]], axis=0)
            block = jnp.dot(turn_back, block, preferred_element_type=F32).astype(BF16)
            x_buf[:, first + b] = block.reshape(count, ROWS, width)
        part = pl.ds(first, len(slabs) // 8)
        outs.append(pltpu.make_async_copy(x_buf.at[:, part], x_hbm.at[:, part], out_sem.at[i]))
        outs[-1].start()

    def trace_freq():
        t_freq[freq] = t_own[...]
        for d in range(1, freq_count):
            send(0, None, lambda d=d: remote(
                t_own, t_freq.at[freq], t_send.at[peer(d)], t_recv.at[freq], par, peer(d)
            ))

    def trace_core():
        for d in range(1, freq_count):
            src = peer(freq_count - d)
            arrived(t_freq.at[src], t_recv.at[src])
        t_mid[...] = jnp.sum(t_freq[...], axis=0)
        send(0, None, lambda: remote(t_mid, t_core, tp_send.at[0], tp_recv.at[0], near, freq))

    def trace_across():
        arrived(t_core, tp_recv.at[0])
        t_half[...] = t_mid[...] + t_core[...]
        send(0, None, lambda: remote(t_half, t_x, tp_send.at[1], tp_recv.at[1], across, freq))

    last = stages - 1
    spread(0)
    pl.semaphore_wait(barrier, freq_count + 1)
    send_spectra(0)
    for i in range(1, stages):
        spread(i)
        send_spectra(i)
    gather(0)
    for i in range(stages):
        if i < last:
            gather(i + 1)
        if i > 2:
            reduce_across(i - 3)
        gather_on(i)
        if i > 0:
            reduce_core(i - 1)
        compute(i)
    trace_freq()
    reduce_core(last)
    first = max(last - 2, 0)
    for i in range(first, last):
        reduce_across(i)
        if i == first:
            back(0)
    reduce_across(last)
    trace_core()
    for i in range(1, stages):
        back(i)
        if i > 1:
            finish(i - 2)
        back_on(i - 1)
        if i == 1:
            trace_across()
    finish(last - 1)
    back_on(last)
    finish(last)
    arrived(t_x, tp_recv.at[1])
    trace_ref[...] = t_half[...] + t_x[...]
    for i, condition, make in pending:
        when(i, condition, lambda make=make: make().wait_send())
    for copy in outs:
        copy.wait()


def inverse_kernel(factor, x_ref, trace_ref, table_ref, probes_ref, out_ref, split_v):
    count, blocks, rows, width = x_ref.shape
    piece, _, sensors = out_ref.shape
    table = table_ref[0]
    trace_est = jnp.sum(trace_ref[...]) * factor
    for r in range(count):
        block = x_ref[r].reshape(blocks * rows, width)
        response = jnp.dot(table, block, preferred_element_type=F32)
        for j in range(width // 128):
            split_v[j, pl.ds(r, piece, stride=count), :] = response[:, 128 * j : 128 * j + 128]
    for j in range(width // 128):
        start, size = 128 * j, min(128, sensors - 128 * j)
        part = split_v[j].reshape(piece, count, 128)[:, :, :size]
        noise = trace_est * probes_ref[:, :, start : start + size].astype(F32)
        out_ref[:, :, start : start + size] = (part + noise).astype(BF16)


def fast_shards(probes, map_real, map_imag, prior_var):
    freq_count = lax.axis_size("freq")
    bins_dev, sensors, params = map_real.shape
    count, _, steps = probes.shape
    stages = -(-bins_dev // GROUP)
    padded = stages * GROUP
    width = -(-sensors // 128) * 128
    pieces = next(n for n in (3, 4, 5, 2, 1) if steps % n == 0)
    forward, inverse = tables(steps, bins_dev, freq_count)
    blocks = inverse.shape[0] // ROWS
    inverse = jnp.asarray(inverse.T.reshape(pieces, steps // pieces, -1), BF16)
    forward = jnp.asarray(forward, BF16)
    swap_out = jnp.asarray(swap_matrix(count, ROWS), BF16)
    swap_in = jnp.asarray(swap_matrix(ROWS, count), BF16)
    by_time = probes.transpose(2, 0, 1)
    vmem, any_place = pl.BlockSpec(memory_space=pltpu.VMEM), pl.BlockSpec(memory_space=pl.ANY)
    dma = pltpu.SemaphoreType.DMA
    block = (freq_count, ROWS, width)
    small = pltpu.VMEM((count, params), F32)
    staged = pltpu.VMEM((stages,) + block, BF16)
    peers, pairs, single = dma((stages, freq_count)), dma((stages, 2)), dma((stages,))
    x, trace = pl.pallas_call(
        functools.partial(exchange_kernel, freq_count),
        out_shape=(
            jax.ShapeDtypeStruct((count, blocks, ROWS, width), BF16),
            jax.ShapeDtypeStruct((count, params), F32),
        ),
        in_specs=[vmem, vmem, vmem, vmem, any_place, any_place, any_place],
        out_specs=(any_place, vmem),
        scratch_shapes=[
            pltpu.VMEM(by_time.shape, BF16),
            pltpu.VMEM((width // 128, steps * count, 128), F32),
            pltpu.VMEM(map_real.shape, BF16),
            pltpu.VMEM(map_imag.shape, BF16),
            pltpu.VMEM((stages, count, ROWS, width), BF16),
            staged,
            pltpu.VMEM((padded,) + block, BF16),
            pltpu.VMEM((padded,) + block, BF16),
            pltpu.VMEM((2, stages) + block, BF16),
            staged,
            staged,
            staged,
            pltpu.VMEM((freq_count, padded, ROWS, width), BF16),
            pltpu.VMEM((count, blocks, ROWS, width), BF16),
            small,
            pltpu.VMEM((freq_count, count, params), F32),
            small,
            small,
            small,
            small,
            dma((pieces,)),
            dma((2,)),
            single,
            peers,
            peers,
            pairs,
            pairs,
            single,
            single,
            pairs,
            pairs,
            single,
            single,
            peers,
            peers,
            pairs,
            pairs,
            single,
            single,
            dma((freq_count,)),
            dma((freq_count,)),
            dma((2,)),
            dma((2,)),
        ],
        compiler_params=pltpu.CompilerParams(
            collective_id=0, has_side_effects=True, vmem_limit_bytes=60 * 1024 * 1024
        ),
        name="exchange",
    )(forward, swap_out, swap_in, prior_var.reshape(1, params), by_time, map_real, map_imag)
    factor = noise_ratio / (count * freq_count * sensors * steps)
    piece = steps // pieces
    result = pl.pallas_call(
        functools.partial(inverse_kernel, factor),
        grid=(pieces,),
        out_shape=jax.ShapeDtypeStruct(by_time.shape, BF16),
        in_specs=[
            pl.BlockSpec(x.shape, lambda n: (0, 0, 0, 0)),
            pl.BlockSpec(trace.shape, lambda n: (0, 0)),
            pl.BlockSpec((1, piece, blocks * ROWS), lambda n: (n, 0, 0)),
            pl.BlockSpec((piece, count, sensors), lambda n: (n, 0, 0)),
        ],
        out_specs=pl.BlockSpec((piece, count, sensors), lambda n: (n, 0, 0)),
        scratch_shapes=[pltpu.VMEM((width // 128, piece * count, 128), F32)],
        compiler_params=pltpu.CompilerParams(vmem_limit_bytes=48 * 1024 * 1024),
        name="inverse",
    )(x, trace, inverse, by_time)
    return result.transpose(1, 2, 0)


def shards(probes, map_real, map_imag, prior_var):
    fits = lax.axis_size("par") == GROUP and lax.axis_size("freq") == 8
    fits = fits and probes.shape[0] == 8 and map_real.shape[0] % 4 in (0, 2) and map_real.shape[0] > 8
    return (fast_shards if fits else plain_shards)(probes, map_real, map_imag, prior_var)


def solution(mesh):
    placed = (P("freq", None, None), P("freq", None, "par"), P("freq", None, "par"), P("par"))
    return jax.shard_map(
        shards, mesh=mesh, in_specs=placed, out_specs=P("freq", None, None), check_vma=False
    )
```
